32 devices in a mesh: dp: 2 (over y), owner: 16 (over z, x, core).
Axes of the slice: x: 2, y: 2, z: 4, core: 2. Of those that a mesh axis runs over, the one named last changes fastest.
Arguments:
- grad_parts: bfloat16 [2, 16, 512, 512], P('dp', None, 'owner'), may hold values from -2.5 to 2.5
- stats: float32 [32, 512, 512], P(('dp', 'owner')), may hold values from -10 to 12, as said below
- roots: bfloat16 [32, 512, 512], P(('dp', 'owner')), may hold values from -0.25 to 0.25
- refresh: int32 [16], P('dp'), may hold values 0 or 1
Outputs:
- new_stats: float32 [32, 512, 512], P(('dp', 'owner'))
- new_roots: bfloat16 [32, 512, 512], P(('dp', 'owner'))
- update: bfloat16 [16, 512, 512], P('dp', 'owner')
The draws below stay inside these ranges and needn't reach their ends.
Inputs may be any that keep to these rules, and one draw needn't show every extreme that they name: Every stats matrix is symmetric positive definite.
All inputs are finite; a program needn't handle non-finite values. No bound on the sum of `refresh` on one device may be relied on, other than what follows from the above.
Results may differ from the reference program's by a relative error of at most 0.015.
Values may be sent and summed in bfloat16 or wider, within the bound.
No kernel may reach another device: no remote copies, remote signals or barrier semaphores. Data moves between devices by JAX's collectives and lax.ppermute only.
A program may use at most 64 MiB of HBM per device.

```python
import jax
import jax.numpy as jnp
from jax import lax

BS = 512
ITERS = 5
BLOCKS = 16
N_DP = 2


def draw_stats(key, part):
    first = jax.random.fold_in(key, 11)
    second = jax.random.fold_in(key, 12)
    third = jax.random.fold_in(key, 13)
    factors = jnp.clip(jax.random.normal(first, (2 * BLOCKS, BS, BS // 4), jnp.float32), -3.0, 3.0)
    scales = jnp.exp(jax.random.uniform(second, (2 * BLOCKS, BS), jnp.float32, -1.1512925, 0.0))
    base = jnp.einsum('mik,mjk->mij', factors, factors) / (BS // 4)
    diagonal = jax.random.uniform(third, (2 * BLOCKS, BS), jnp.float32, 1.0, 2.0) * scales * scales
    eye = jnp.eye(BS, dtype=jnp.float32)
    return scales[:, :, None] * scales[:, None, :] * base + diagonal[:, :, None] * eye


def plant(entries, stream_key, least, top_value):
    shape = entries.shape
    index_at = [jax.random.randint(jax.random.fold_in(stream_key, axis), (), 0, shape[axis]) for axis in range(len(shape))]
    entries = entries.at[tuple(index_at)].set(least)
    longest = shape.index(max(shape))
    index_at[longest] = (index_at[longest] + 1) % shape[longest]
    return entries.at[tuple(index_at)].set(top_value)


def raised(drawn, stream_key, source, target, shards_of, factor):
    def block_of(dim):
        return (jnp.arange(drawn.shape[dim]) // (drawn.shape[dim] // shards_of)).reshape((-1,) + (1,) * (drawn.ndim - 1 - dim))

    first = jax.random.permutation(stream_key, shards_of)[block_of(target)]
    second = (block_of(target) + shards_of // 2) % shards_of
    return jnp.where((block_of(source) == first) | (block_of(source) == second), factor * drawn, drawn)


def levels(stream_key, shape, split, least, high):
    level = 1.0
    for position, shards_of in split:
        steps = jax.random.uniform(jax.random.fold_in(jax.random.fold_in(stream_key, 6), position), (shards_of,), jnp.float32, least / len(split), high / len(split))
        level = level * jnp.repeat(jnp.exp(steps), shape[position] // shards_of).reshape((-1,) + (1,) * (len(shape) - 1 - position))
    return level


def normal_values(key, shape, width, reach, cuts=(), held_as=jnp.bfloat16):
    values = width * jax.random.normal(key, shape, jnp.float32)
    if cuts:
        values = values * levels(key, shape, cuts, -0.22, 0.18)
    return jnp.clip(values, -reach, reach).astype(held_as)


def bell_draw_with(own_key, extent, deviation, bound, cuts, heavy, kind=jnp.bfloat16):
    entries = deviation * jax.random.normal(own_key, extent, jnp.float32)
    if cuts:
        entries = entries * levels(own_key, extent, cuts, -0.22, 0.18)
    return jnp.clip(raised(entries, jax.random.fold_in(own_key, 3), *heavy), -bound, bound).astype(kind)


def setup_inputs(seed: int = 0) -> dict:
    seeds = jax.random.split(jax.random.key(seed), 5)
    grad_parts = bell_draw_with(seeds[0], (N_DP, BLOCKS, BS, BS), 0.35, 2.5, ((0, 2), (2, 16)), (0, 1, 2, 2.0))
    stats = draw_stats(jax.random.fold_in(seeds[4], 71), 0)
    roots = normal_values(seeds[2], (2 * BLOCKS, BS, BS), BS ** -0.5, 0.25, ((0, 32),))
    refresh = plant((jax.random.randint(seeds[3], (BLOCKS,), 0, 2) < 1).astype(jnp.int32), jax.random.fold_in(seeds[3], 1), 0, 1)
    return dict(grad_parts=grad_parts, stats=stats, roots=roots, refresh=refresh)


BETA = 0.8

def inverse_root(matrix):
    size = matrix.shape[0]
    eye = jnp.eye(size, dtype=jnp.float32)
    scale = jnp.sqrt(jnp.sum(matrix * matrix) + 1e-06)
    current = matrix / scale
    result = eye * scale ** (-0.25)
    for step in range(ITERS):
        factor = (5.0 * eye - current) / 4.0
        result = jnp.dot(result, factor, precision=lax.Precision.HIGHEST)
        if step + 1 < ITERS:
            square = jnp.dot(factor, factor, precision=lax.Precision.HIGHEST)
            fourth = jnp.dot(square, square, precision=lax.Precision.HIGHEST)
            current = jnp.dot(fourth, current, precision=lax.Precision.HIGHEST)
    return result

def reference(grad_parts, stats, roots, refresh):
    grad = lax.optimization_barrier(jnp.sum(grad_parts.astype(jnp.float32), axis=0)).astype(jnp.bfloat16)
    pair_stats = stats.reshape(BLOCKS, 2, BS, BS)
    pair_roots = roots.reshape(BLOCKS, 2, BS, BS)

    def per_block(items):
        block, old_stats, old_roots, flag = items
        wide = block.astype(jnp.float32)
        left = jnp.dot(wide, wide.T, precision=lax.Precision.HIGHEST) / BS
        right = jnp.dot(wide.T, wide, precision=lax.Precision.HIGHEST) / BS
        fresh = BETA * old_stats + (1.0 - BETA) * jnp.stack([left, right])
        solved = jnp.stack([inverse_root(fresh[0]), inverse_root(fresh[1])])
        chosen = jnp.where(flag == 1, solved.astype(jnp.bfloat16), old_roots)
        product = jnp.dot(old_roots[0], block, preferred_element_type=jnp.float32).astype(jnp.bfloat16)
        result = jnp.dot(product, old_roots[1], preferred_element_type=jnp.float32).astype(jnp.bfloat16)
        return (fresh, chosen, result)
    fresh, chosen, update = lax.map(per_block, (grad, pair_stats, pair_roots, refresh))
    return (fresh.reshape(2 * BLOCKS, BS, BS), chosen.reshape(2 * BLOCKS, BS, BS), update)
```

```python
import jax
import jax.numpy as jnp
from jax import lax
from jax.experimental import pallas as pl
from jax.experimental.pallas import tpu as pltpu
from jax.sharding import PartitionSpec as P

ITERS = 5
BETA = 0.8


def dot(a, b, dims=((1,), (0,))):
    return lax.dot_general(a, b, (dims, ((), ())), preferred_element_type=jnp.float32)


def product_kernel(core, mine, other, root, partner, whole, portion):
    @pl.when(core[0] == 0)
    def _():
        run_side(0, mine, other, root, partner, whole, portion)

    @pl.when(core[0] == 1)
    def _():
        run_side(1, other, mine, partner, root, whole, portion)


def run_side(side, first, second, left, right, whole, portion):
    chips, rows, width = first.shape
    for chip in range(chips):
        whole[pl.ds(2 * chip * rows, rows), :] = first[chip]
        whole[pl.ds((2 * chip + 1) * rows, rows), :] = second[chip]
    picked = jnp.concatenate(
        [left[pl.ds((2 * chip + side) * rows, rows), :] for chip in range(chips)], axis=0
    )
    product = dot(picked, whole[...]).astype(jnp.bfloat16)
    portion[...] = dot(product, right[...]).astype(jnp.bfloat16)


def root_kernel(flags, whole, stats, root, fresh, chosen, n, y, t, nb, yb):
    width = whole.shape[0]
    weight = (1.0 - BETA) / width

    @pl.when(flags[0] == 0)
    def _():
        fresh[...] = BETA * stats[...] + weight * dot(whole[...], whole[...], ((1,), (1,)))

    @pl.when(flags[0] == 1)
    def _():
        fresh[...] = BETA * stats[...] + weight * dot(whole[...], whole[...], ((0,), (0,)))

    @pl.when(flags[1] == 1)
    def _():
        value = fresh[...]
        total = jnp.sum(jnp.sum(value * value, axis=0, keepdims=True), axis=1, keepdims=True) + 1e-06
        start = value * (0.25 * lax.rsqrt(total))
        n[...] = start
        y[...] = -start
        nb[...] = start.astype(jnp.bfloat16)
        yb[...] = (-start).astype(jnp.bfloat16)

        def square_step():
            t[...] = dot(nb[...], nb[...]) - 2.5 * n[...]
            low = t[...].astype(jnp.bfloat16)
            return (dot(low, low) + 3.125 * t[...]).astype(jnp.bfloat16)

        def advance(grown, first):
            fourth = square_step()
            old = nb[...]
            if not first:
                move = 1.25 * y[...] - grown * n[...] - dot(yb[...], old)
                y[...] = move
                yb[...] = move.astype(jnp.bfloat16)
            new = dot(fourth, old) + 2.44140625 * n[...]
            n[...] = new
            nb[...] = new.astype(jnp.bfloat16)

        advance(1.0, True)

        def body(step, grown):
            advance(grown, False)
            return 1.25 * grown

        grown = lax.fori_loop(1, ITERS - 1, body, jnp.float32(1.25))
        last = 1.25 * y[...] - grown * n[...] - dot(yb[...], nb[...])
        shape = (width, width)
        diagonal = lax.broadcasted_iota(jnp.int32, shape, 0) == lax.broadcasted_iota(jnp.int32, shape, 1)
        scale = lax.rsqrt(jnp.sqrt(jnp.sqrt(total)))
        chosen[...] = ((last + jnp.where(diagonal, 1.25 * grown, 0.0)) * scale).astype(jnp.bfloat16)

    @pl.when(flags[1] != 1)
    def _():
        chosen[...] = root[...]


def local(grad_parts, stats, roots, refresh):
    groups = lax.axis_size("dp")
    owners = lax.axis_size("owner")
    chips = owners // 2
    _, total, rows, width = grad_parts.shape
    blocks = total // groups
    group = lax.axis_index("dp")
    owner = lax.axis_index("owner")
    core = owner % 2
    flag = lax.dynamic_index_in_dim(refresh, owner // 2, 0, keepdims=False)
    swap = [(source, source ^ 1) for source in range(owners)]
    partner = lax.ppermute(roots[0], "owner", swap)

    parts = grad_parts.reshape(groups, blocks, rows, width)
    added = lax.dynamic_index_in_dim(parts, group, 0, keepdims=False).astype(jnp.float32)
    for shift in range(1, groups):
        piece = lax.dynamic_index_in_dim(parts, (group + shift) % groups, 0, keepdims=False)
        pairs = [(source, (source + shift) % groups) for source in range(groups)]
        added = added + lax.ppermute(piece, "dp", pairs).astype(jnp.float32)
    grad = added.astype(jnp.bfloat16)

    members = [[2 * chip + side for chip in range(chips)] for side in range(2)]

    def exchange(value):
        return lax.all_to_all(value, "owner", 0, 0, axis_index_groups=members, tiled=True)

    mine = exchange(grad)
    other = lax.ppermute(mine, "owner", swap)

    vmem = pl.BlockSpec(memory_space=pltpu.VMEM)
    smem = pl.BlockSpec(memory_space=pltpu.SMEM)
    square = (width, width)
    whole, portion = pl.pallas_call(
        product_kernel,
        out_shape=(
            jax.ShapeDtypeStruct(square, jnp.bfloat16),
            jax.ShapeDtypeStruct((chips * rows, width), jnp.bfloat16),
        ),
        in_specs=[smem, vmem, vmem, vmem, vmem],
        out_specs=(vmem, vmem),
        name="product",
    )(core[None].astype(jnp.int32), mine, other, roots[0], partner)
    update = exchange(portion.reshape(chips, rows, width))

    fresh, chosen = pl.pallas_call(
        root_kernel,
        out_shape=(
            jax.ShapeDtypeStruct(square, jnp.float32),
            jax.ShapeDtypeStruct(square, jnp.bfloat16),
        ),
        in_specs=[smem, vmem, vmem, vmem],
        out_specs=(vmem, vmem),
        scratch_shapes=[
            pltpu.VMEM(square, jnp.float32),
            pltpu.VMEM(square, jnp.float32),
            pltpu.VMEM(square, jnp.float32),
            pltpu.VMEM(square, jnp.bfloat16),
            pltpu.VMEM(square, jnp.bfloat16),
        ],
        name="root",
    )(jnp.stack([core, flag]).astype(jnp.int32), whole, stats[0], roots[0])
    return (fresh[None], chosen[None], update)


def solution(mesh):
    return jax.shard_map(
        local,
        mesh=mesh,
        in_specs=(
            P("dp", None, "owner", None),
            P(("dp", "owner"), None, None),
            P(("dp", "owner"), None, None),
            P("dp"),
        ),
        out_specs=(
            P(("dp", "owner"), None, None),
            P(("dp", "owner"), None, None),
            P("dp", "owner", None),
        ),
        check_vma=False,
    )
```

```python
import jax
import jax.numpy as jnp
from jax import lax
from jax.experimental import pallas as pl
from jax.experimental.pallas import tpu as pltpu
from jax.sharding import PartitionSpec as P

ITERS = 5
BETA = 0.8
VMEM = pl.BlockSpec(memory_space=pltpu.VMEM)
SMEM = pl.BlockSpec(memory_space=pltpu.SMEM)
PARAMS = pltpu.CompilerParams(vmem_limit_bytes=16 * 2**20)


def dot(a, b, dims=((1,), (0,))):
    return lax.dot_general(a, b, (dims, ((), ())), preferred_element_type=jnp.float32)


def add_kernel(terms, out):
    out[...] = (terms[0].astype(jnp.float32) + terms[1].astype(jnp.float32)).astype(jnp.bfloat16)


def product_kernel(mine, other, root, partner, whole, portion):
    side = lax.axis_index("owner") % 2

    @pl.when(side == 0)
    def _():
        run_side(0, mine, other, root, partner, whole, portion)

    @pl.when(side == 1)
    def _():
        run_side(1, other, mine, partner, root, whole, portion)


def run_side(side, first, second, left, right, whole, portion):
    chips, rows, width = first.shape
    for chip in range(chips):
        whole[pl.ds(2 * chip * rows, rows), :] = first[chip]
        whole[pl.ds((2 * chip + 1) * rows, rows), :] = second[chip]
    picked = jnp.concatenate(
        [left[pl.ds((2 * chip + side) * rows, rows), :] for chip in range(chips)], axis=0
    )
    product = dot(picked, whole[...]).astype(jnp.bfloat16)
    portion[...] = dot(product, right[...]).astype(jnp.bfloat16)


def root_kernel(flags, whole, stats, root, fresh, chosen, n, y, t, nb, yb):
    width = whole.shape[0]
    weight = (1.0 - BETA) / width
    owner = lax.axis_index("owner")
    flag = flags[owner // 2]

    @pl.when(owner % 2 == 0)
    def _():
        fresh[...] = BETA * stats[...] + weight * dot(whole[...], whole[...], ((1,), (1,)))

    @pl.when(owner % 2 == 1)
    def _():
        fresh[...] = BETA * stats[...] + weight * dot(whole[...], whole[...], ((0,), (0,)))

    @pl.when(flag == 1)
    def _():
        value = fresh[...]
        total = jnp.sum(jnp.sum(value * value, axis=0, keepdims=True), axis=1, keepdims=True) + 1e-06
        start = value * (0.25 * lax.rsqrt(total))
        n[...] = start
        y[...] = -start
        nb[...] = start.astype(jnp.bfloat16)
        yb[...] = (-start).astype(jnp.bfloat16)

        def advance(grown, first):
            t[...] = dot(nb[...], nb[...]) - 2.5 * n[...]
            low = t[...].astype(jnp.bfloat16)
            fourth = (dot(low, low) + 3.125 * t[...]).astype(jnp.bfloat16)
            old = nb[...]
            if not first:
                move = 1.25 * y[...] - grown * n[...] - dot(yb[...], old)
                y[...] = move
                yb[...] = move.astype(jnp.bfloat16)
            new = dot(fourth, old) + 2.44140625 * n[...]
            n[...] = new
            nb[...] = new.astype(jnp.bfloat16)

        advance(1.0, True)

        def body(step, grown):
            advance(grown, False)
            return 1.25 * grown

        grown = lax.fori_loop(1, ITERS - 1, body, jnp.float32(1.25))
        last = 1.25 * y[...] - grown * n[...] - dot(yb[...], nb[...])
        shape = (width, width)
        diagonal = lax.broadcasted_iota(jnp.int32, shape, 0) == lax.broadcasted_iota(jnp.int32, shape, 1)
        scale = lax.rsqrt(jnp.sqrt(jnp.sqrt(total)))
        chosen[...] = ((last + jnp.where(diagonal, 1.25 * grown, 0.0)) * scale).astype(jnp.bfloat16)

    @pl.when(flag != 1)
    def _():
        chosen[...] = root[...]


def local(grad_parts, stats, roots, refresh):
    groups = lax.axis_size("dp")
    owners = lax.axis_size("owner")
    chips = owners // 2
    _, total, rows, width = grad_parts.shape
    blocks = total // groups
    group = lax.axis_index("dp")
    swap = [(source, source ^ 1) for source in range(owners)]
    partner = lax.ppermute(roots[0], "owner", swap)

    sides = range(2)
    members = [[2 * chip + side for chip in range(chips)] for side in sides]

    def exchange(value):
        return lax.all_to_all(value, "owner", 0, 0, axis_index_groups=members, tiled=True)

    if groups == 2:
        spread = [[pair * owners + one for pair in range(groups) for one in each] for each in members]
        terms = lax.all_to_all(
            grad_parts[0], ("dp", "owner"), 0, 0, axis_index_groups=spread, tiled=True
        ).reshape(groups, chips, rows, width)
        mine = pl.pallas_call(
            add_kernel,
            out_shape=jax.ShapeDtypeStruct((chips, rows, width), jnp.bfloat16),
            in_specs=[VMEM],
            out_specs=VMEM,
            compiler_params=PARAMS,
            name="add",
        )(terms)
    else:
        parts = grad_parts.reshape(groups, blocks, rows, width)
        added = lax.dynamic_index_in_dim(parts, group, 0, keepdims=False).astype(jnp.float32)
        for shift in range(1, groups):
            piece = lax.dynamic_index_in_dim(parts, (group + shift) % groups, 0, keepdims=False)
            pairs = [(source, (source + shift) % groups) for source in range(groups)]
            added = added + lax.ppermute(piece, "dp", pairs).astype(jnp.float32)
        mine = exchange(added.astype(jnp.bfloat16))
    other = lax.ppermute(mine, "owner", swap)

    square = (width, width)
    whole, portion = pl.pallas_call(
        product_kernel,
        out_shape=(
            jax.ShapeDtypeStruct(square, jnp.bfloat16),
            jax.ShapeDtypeStruct((chips * rows, width), jnp.bfloat16),
        ),
        in_specs=[VMEM, VMEM, VMEM, VMEM],
        out_specs=(VMEM, VMEM),
        compiler_params=PARAMS,
        name="product",
    )(mine, other, roots[0], partner)
    update = exchange(portion.reshape(chips, rows, width))

    fresh, chosen = pl.pallas_call(
        root_kernel,
        out_shape=(
            jax.ShapeDtypeStruct(square, jnp.float32),
            jax.ShapeDtypeStruct(square, jnp.bfloat16),
        ),
        in_specs=[SMEM, VMEM, VMEM, VMEM],
        out_specs=(VMEM, VMEM),
        scratch_shapes=[
            pltpu.VMEM(square, jnp.float32),
            pltpu.VMEM(square, jnp.float32),
            pltpu.VMEM(square, jnp.float32),
            pltpu.VMEM(square, jnp.bfloat16),
            pltpu.VMEM(square, jnp.bfloat16),
        ],
        compiler_params=PARAMS,
        name="root",
    )(refresh, whole, stats[0], roots[0])
    return (fresh[None], chosen[None], update)


def solution(mesh):
    return jax.shard_map(
        local,
        mesh=mesh,
        in_specs=(
            P("dp", None, "owner", None),
            P(("dp", "owner"), None, None),
            P(("dp", "owner"), None, None),
            P("dp"),
        ),
        out_specs=(
            P(("dp", "owner"), None, None),
            P(("dp", "owner"), None, None),
            P("dp", "owner", None),
        ),
        check_vma=False,
    )
```

```python
import jax
import jax.numpy as jnp
from jax import lax
from jax.experimental import pallas as pl
from jax.experimental.pallas import tpu as pltpu
from jax.sharding import PartitionSpec as P

ITERS = 5
BETA = 0.8


def order(side, chips):
    return [(step + side * (chips // 2)) % chips for step in range(chips)]

VMEM = pl.BlockSpec(memory_space=pltpu.VMEM)
HBM = pl.BlockSpec(memory_space=pltpu.HBM)
PARAMS = pltpu.CompilerParams(vmem_limit_bytes=16 * 2**20)


def dot(a, b, dims=((1,), (0,))):
    return lax.dot_general(a, b, (dims, ((), ())), preferred_element_type=jnp.float32)


def add_kernel(terms, out):
    out[...] = (terms[0].astype(jnp.float32) + terms[1].astype(jnp.float32)).astype(jnp.bfloat16)


def product_kernel(mine, other, root, partner, refresh, whole, portion):
    side = lax.axis_index("owner") % 2

    @pl.when(side == 0)
    def _():
        run_side(0, mine, other, root, partner, whole, portion)

    @pl.when(side == 1)
    def _():
        run_side(1, other, mine, partner, root, whole, portion)


def run_side(side, first, second, left, right, whole, portion):
    chips, rows, width = first.shape
    for chip in range(chips):
        whole[pl.ds(2 * chip * rows, rows), :] = first[chip]
        whole[pl.ds((2 * chip + 1) * rows, rows), :] = second[chip]
    picked = jnp.concatenate(
        [left[pl.ds((2 * chip + side) * rows, rows), :] for chip in order(side, chips)], axis=0
    )
    product = dot(picked, whole[...]).astype(jnp.bfloat16)
    portion[...] = dot(product, right[...]).astype(jnp.bfloat16)


def place_kernel(moved, update, sent):
    chips = moved.shape[0]
    for side in range(2):

        @pl.when(lax.axis_index("owner") % 2 == side)
        def _():
            copies = [
                pltpu.make_async_copy(moved.at[step], update.at[chip], sent.at[step])
                for step, chip in enumerate(order(side, chips))
            ]
            for copy in copies:
                copy.start()
            for copy in copies:
                copy.wait()


def root_kernel(refresh, whole, stats, root, out, chosen, fresh, n, y, t, nb, yb, flags, sent):
    width = whole.shape[0]
    weight = (1.0 - BETA) / width
    owner = lax.axis_index("owner")
    fetch = pltpu.make_async_copy(refresh, flags, sent.at[0])
    fetch.start()

    @pl.when(owner % 2 == 0)
    def _():
        fresh[...] = BETA * stats[...] + weight * dot(whole[...], whole[...], ((1,), (1,)))

    @pl.when(owner % 2 == 1)
    def _():
        fresh[...] = BETA * stats[...] + weight * dot(whole[...], whole[...], ((0,), (0,)))

    store = pltpu.make_async_copy(fresh, out, sent.at[1])
    store.start()
    fetch.wait()
    flag = flags[owner // 2]

    @pl.when(flag == 1)
    def _():
        value = fresh[...]
        total = jnp.sum(jnp.sum(value * value, axis=0, keepdims=True), axis=1, keepdims=True) + 1e-06
        start = value * (0.25 * lax.rsqrt(total))
        n[...] = start
        y[...] = -start
        nb[...] = start.astype(jnp.bfloat16)
        yb[...] = (-start).astype(jnp.bfloat16)

        def advance(grown, first):
            t[...] = dot(nb[...], nb[...]) - 2.5 * n[...]
            low = t[...].astype(jnp.bfloat16)
            fourth = (dot(low, low) + 3.125 * t[...]).astype(jnp.bfloat16)
            old = nb[...]
            if not first:
                move = 1.25 * y[...] - grown * n[...] - dot(yb[...], old)
                y[...] = move
                yb[...] = move.astype(jnp.bfloat16)
            new = dot(fourth, old) + 2.44140625 * n[...]
            n[...] = new
            nb[...] = new.astype(jnp.bfloat16)

        advance(1.0, True)

        def body(step, grown):
            advance(grown, False)
            return 1.25 * grown

        grown = lax.fori_loop(1, ITERS - 1, body, jnp.float32(1.25))
        last = 1.25 * y[...] - grown * n[...] - dot(yb[...], nb[...])
        shape = (width, width)
        diagonal = lax.broadcasted_iota(jnp.int32, shape, 0) == lax.broadcasted_iota(jnp.int32, shape, 1)
        scale = lax.rsqrt(jnp.sqrt(jnp.sqrt(total)))
        chosen[...] = ((last + jnp.where(diagonal, 1.25 * grown, 0.0)) * scale).astype(jnp.bfloat16)

    @pl.when(flag != 1)
    def _():
        chosen[...] = root[...]

    store.wait()


def local(grad_parts, stats, roots, refresh):
    groups = lax.axis_size("dp")
    owners = lax.axis_size("owner")
    chips = owners // 2
    _, total, rows, width = grad_parts.shape
    blocks = total // groups
    group = lax.axis_index("dp")
    swap = [(source, source ^ 1) for source in range(owners)]
    partner = lax.ppermute(roots[0], "owner", swap)

    sides = range(2)
    members = [[2 * chip + side for chip in range(chips)] for side in sides]

    def exchange(value):
        return lax.all_to_all(value, "owner", 0, 0, axis_index_groups=members, tiled=True)

    if groups == 2:
        spread = [[pair * owners + one for pair in range(groups) for one in each] for each in members]
        terms = lax.all_to_all(
            grad_parts[0], ("dp", "owner"), 0, 0, axis_index_groups=spread, tiled=True
        ).reshape(groups, chips, rows, width)
        mine = pl.pallas_call(
            add_kernel,
            out_shape=jax.ShapeDtypeStruct((chips, rows, width), jnp.bfloat16),
            in_specs=[VMEM],
            out_specs=VMEM,
            compiler_params=PARAMS,
            name="add",
        )(terms)
    else:
        parts = grad_parts.reshape(groups, blocks, rows, width)
        added = lax.dynamic_index_in_dim(parts, group, 0, keepdims=False).astype(jnp.float32)
        for shift in range(1, groups):
            piece = lax.dynamic_index_in_dim(parts, (group + shift) % groups, 0, keepdims=False)
            pairs = [(source, (source + shift) % groups) for source in range(groups)]
            added = added + lax.ppermute(piece, "dp", pairs).astype(jnp.float32)
        mine = exchange(added.astype(jnp.bfloat16))
    other = lax.ppermute(mine, "owner", swap)

    square = (width, width)
    whole, portion = pl.pallas_call(
        product_kernel,
        out_shape=(
            jax.ShapeDtypeStruct(square, jnp.bfloat16),
            jax.ShapeDtypeStruct((chips * rows, width), jnp.bfloat16),
        ),
        in_specs=[VMEM, VMEM, VMEM, VMEM, HBM],
        out_specs=(VMEM, VMEM),
        compiler_params=PARAMS,
        name="product",
    )(mine, other, roots[0], partner, refresh)
    shape = (chips, rows, width)
    served = [[2 * chip + side for chip in order(side, chips)] for side in range(2)]
    moved = lax.all_to_all(
        portion.reshape(shape), "owner", 0, 0, axis_index_groups=served, tiled=True
    )
    update = pl.pallas_call(
        place_kernel,
        out_shape=jax.ShapeDtypeStruct(shape, jnp.bfloat16),
        in_specs=[VMEM],
        out_specs=HBM,
        scratch_shapes=[pltpu.SemaphoreType.DMA((chips,))],
        compiler_params=PARAMS,
        name="place",
    )(moved)

    fresh, chosen = pl.pallas_call(
        root_kernel,
        out_shape=(
            jax.ShapeDtypeStruct(square, jnp.float32),
            jax.ShapeDtypeStruct(square, jnp.bfloat16),
        ),
        in_specs=[HBM, VMEM, VMEM, VMEM],
        out_specs=(HBM, VMEM),
        scratch_shapes=[
            pltpu.VMEM(square, jnp.float32),
            pltpu.VMEM(square, jnp.float32),
            pltpu.VMEM(square, jnp.float32),
            pltpu.VMEM(square, jnp.float32),
            pltpu.VMEM(square, jnp.bfloat16),
            pltpu.VMEM(square, jnp.bfloat16),
            pltpu.SMEM(refresh.shape, jnp.int32),
            pltpu.SemaphoreType.DMA((2,)),
        ],
        compiler_params=PARAMS,
        name="root",
    )(refresh, whole, stats[0], roots[0])
    return (fresh[None], chosen[None], update)


def solution(mesh):
    return jax.shard_map(
        local,
        mesh=mesh,
        in_specs=(
            P("dp", None, "owner", None),
            P(("dp", "owner"), None, None),
            P(("dp", "owner"), None, None),
            P("dp"),
        ),
        out_specs=(
            P(("dp", "owner"), None, None),
            P(("dp", "owner"), None, None),
            P("dp", "owner", None),
        ),
        check_vma=False,
    )
```

```python
import jax
import jax.numpy as jnp
from jax import lax
from jax.experimental import pallas as pl
from jax.experimental.pallas import tpu as pltpu
from jax.sharding import PartitionSpec as P

ITERS = 5
BETA = 0.8


def order(side, chips):
    half = chips // 2
    return [
        (turn ^ side) * half + (step + (turn * (1 - side)) * (half // 2)) % half for turn in range(2) for step in range(half)
    ]

VMEM = pl.BlockSpec(memory_space=pltpu.VMEM)
HBM = pl.BlockSpec(memory_space=pltpu.HBM)
PARAMS = pltpu.CompilerParams(vmem_limit_bytes=16 * 2**20)


def dot(a, b, dims=((1,), (0,))):
    return lax.dot_general(a, b, (dims, ((), ())), preferred_element_type=jnp.float32)


def add_kernel(terms, out):
    out[...] = (terms[0].astype(jnp.float32) + terms[1].astype(jnp.float32)).astype(jnp.bfloat16)


def product_kernel(mine, other, root, partner, refresh, whole, portion):
    side = lax.axis_index("owner") % 2

    @pl.when(side == 0)
    def _():
        run_side(0, mine, other, root, partner, whole, portion)

    @pl.when(side == 1)
    def _():
        run_side(1, other, mine, partner, root, whole, portion)


def run_side(side, first, second, left, right, whole, portion):
    chips, rows, width = first.shape
    for chip in range(chips):
        whole[pl.ds(2 * chip * rows, rows), :] = first[chip]
        whole[pl.ds((2 * chip + 1) * rows, rows), :] = second[chip]
    picked = jnp.concatenate(
        [left[pl.ds((2 * chip + side) * rows, rows), :] for chip in order(side, chips)], axis=0
    )
    product = dot(picked, whole[...]).astype(jnp.bfloat16)
    portion[...] = dot(product, right[...]).astype(jnp.bfloat16)


def place_kernel(moved, update, sent):
    chips = moved.shape[0]
    for side in range(2):

        @pl.when(lax.axis_index("owner") % 2 == side)
        def _():
            copies = [
                pltpu.make_async_copy(moved.at[step], update.at[chip], sent.at[step])
                for step, chip in enumerate(order(side, chips))
            ]
            for copy in copies:
                copy.start()
            for copy in copies:
                copy.wait()


def root_kernel(refresh, whole, stats, root, out, chosen, fresh, n, y, t, nb, yb, flags, sent):
    width = whole.shape[0]
    weight = (1.0 - BETA) / width
    owner = lax.axis_index("owner")
    fetch = pltpu.make_async_copy(refresh, flags, sent.at[0])
    fetch.start()

    @pl.when(owner % 2 == 0)
    def _():
        fresh[...] = BETA * stats[...] + weight * dot(whole[...], whole[...], ((1,), (1,)))

    @pl.when(owner % 2 == 1)
    def _():
        fresh[...] = BETA * stats[...] + weight * dot(whole[...], whole[...], ((0,), (0,)))

    store = pltpu.make_async_copy(fresh, out, sent.at[1])
    store.start()
    fetch.wait()
    flag = flags[owner // 2]

    @pl.when(flag == 1)
    def _():
        value = fresh[...]
        total = jnp.sum(jnp.sum(value * value, axis=0, keepdims=True), axis=1, keepdims=True) + 1e-06
        start = value * (0.25 * lax.rsqrt(total))
        n[...] = start
        y[...] = -start
        nb[...] = start.astype(jnp.bfloat16)
        yb[...] = (-start).astype(jnp.bfloat16)

        def advance(grown, first):
            t[...] = dot(nb[...], nb[...]) - 2.5 * n[...]
            low = t[...].astype(jnp.bfloat16)
            fourth = (dot(low, low) + 3.125 * t[...]).astype(jnp.bfloat16)
            old = nb[...]
            if not first:
                move = 1.25 * y[...] - grown * n[...] - dot(yb[...], old)
                y[...] = move
                yb[...] = move.astype(jnp.bfloat16)
            new = dot(fourth, old) + 2.44140625 * n[...]
            n[...] = new
            nb[...] = new.astype(jnp.bfloat16)

        advance(1.0, True)

        def body(step, grown):
            advance(grown, False)
            return 1.25 * grown

        grown = lax.fori_loop(1, ITERS - 1, body, jnp.float32(1.25))
        last = 1.25 * y[...] - grown * n[...] - dot(yb[...], nb[...])
        shape = (width, width)
        diagonal = lax.broadcasted_iota(jnp.int32, shape, 0) == lax.broadcasted_iota(jnp.int32, shape, 1)
        scale = lax.rsqrt(jnp.sqrt(jnp.sqrt(total)))
        chosen[...] = ((last + jnp.where(diagonal, 1.25 * grown, 0.0)) * scale).astype(jnp.bfloat16)

    @pl.when(flag != 1)
    def _():
        chosen[...] = root[...]

    store.wait()


def local(grad_parts, stats, roots, refresh):
    groups = lax.axis_size("dp")
    owners = lax.axis_size("owner")
    chips = owners // 2
    _, total, rows, width = grad_parts.shape
    blocks = total // groups
    group = lax.axis_index("dp")
    swap = [(source, source ^ 1) for source in range(owners)]
    partner = lax.ppermute(roots[0], "owner", swap)

    sides = range(2)
    members = [[2 * chip + side for chip in range(chips)] for side in sides]

    def exchange(value):
        return lax.all_to_all(value, "owner", 0, 0, axis_index_groups=members, tiled=True)

    if groups == 2:
        spread = [[pair * owners + one for pair in range(groups) for one in each] for each in members]
        terms = lax.all_to_all(
            grad_parts[0], ("dp", "owner"), 0, 0, axis_index_groups=spread, tiled=True
        ).reshape(groups, chips, rows, width)
        mine = pl.pallas_call(
            add_kernel,
            out_shape=jax.ShapeDtypeStruct((chips, rows, width), jnp.bfloat16),
            in_specs=[VMEM],
            out_specs=VMEM,
            compiler_params=PARAMS,
            name="add",
        )(terms)
    else:
        parts = grad_parts.reshape(groups, blocks, rows, width)
        added = lax.dynamic_index_in_dim(parts, group, 0, keepdims=False).astype(jnp.float32)
        for shift in range(1, groups):
            piece = lax.dynamic_index_in_dim(parts, (group + shift) % groups, 0, keepdims=False)
            pairs = [(source, (source + shift) % groups) for source in range(groups)]
            added = added + lax.ppermute(piece, "dp", pairs).astype(jnp.float32)
        mine = exchange(added.astype(jnp.bfloat16))
    other = lax.ppermute(mine, "owner", swap)

    square = (width, width)
    whole, portion = pl.pallas_call(
        product_kernel,
        out_shape=(
            jax.ShapeDtypeStruct(square, jnp.bfloat16),
            jax.ShapeDtypeStruct((chips * rows, width), jnp.bfloat16),
        ),
        in_specs=[VMEM, VMEM, VMEM, VMEM, HBM],
        out_specs=(VMEM, VMEM),
        compiler_params=PARAMS,
        name="product",
    )(mine, other, roots[0], partner, refresh)
    shape = (chips, rows, width)
    served = [[2 * chip + side for chip in order(side, chips)] for side in range(2)]
    moved = lax.all_to_all(
        portion.reshape(shape), "owner", 0, 0, axis_index_groups=served, tiled=True
    )
    update = pl.pallas_call(
        place_kernel,
        out_shape=jax.ShapeDtypeStruct(shape, jnp.bfloat16),
        in_specs=[VMEM],
        out_specs=HBM,
        scratch_shapes=[pltpu.SemaphoreType.DMA((chips,))],
        compiler_params=PARAMS,
        name="place",
    )(moved)

    fresh, chosen = pl.pallas_call(
        root_kernel,
        out_shape=(
            jax.ShapeDtypeStruct(square, jnp.float32),
            jax.ShapeDtypeStruct(square, jnp.bfloat16),
        ),
        in_specs=[HBM, VMEM, VMEM, VMEM],
        out_specs=(HBM, VMEM),
        scratch_shapes=[
            pltpu.VMEM(square, jnp.float32),
            pltpu.VMEM(square, jnp.float32),
            pltpu.VMEM(square, jnp.float32),
            pltpu.VMEM(square, jnp.float32),
            pltpu.VMEM(square, jnp.bfloat16),
            pltpu.VMEM(square, jnp.bfloat16),
            pltpu.SMEM(refresh.shape, jnp.int32),
            pltpu.SemaphoreType.DMA((2,)),
        ],
        compiler_params=PARAMS,
        name="root",
    )(refresh, whole, stats[0], roots[0])
    return (fresh[None], chosen[None], update)


def solution(mesh):
    return jax.shard_map(
        local,
        mesh=mesh,
        in_specs=(
            P("dp", None, "owner", None),
            P(("dp", "owner"), None, None),
            P(("dp", "owner"), None, None),
            P("dp"),
        ),
        out_specs=(
            P(("dp", "owner"), None, None),
            P(("dp", "owner"), None, None),
            P("dp", "owner", None),
        ),
        check_vma=False,
    )
```
